256 devices in a mesh: feat: 64 (over y, z, core), samp: 4 (over x).
Axes of the slice: x: 4, y: 4, z: 8, core: 2. Of those that a mesh axis runs over, the one named last changes fastest.
Arguments:
- design: bfloat16 [14336, 65536], P('samp', 'feat'), may hold values from -0.125 to 0.125
- targets: bfloat16 [14336, 128], P('samp'), may hold values from -26 to 26
- warm_start: float32 [65536, 128], P('feat'), may hold values from -0.6 to 0.6
- active_mask: int32 [2, 65536], P(None, 'feat'), may hold values 0 or 1
- penalty_index: int32 [1], replicated, may hold values from 0 to 7
Outputs:
- coefficients: float32 [65536, 128], P('feat')
- correlations: float32 [3, 65536], P(None, 'feat')
- relative_gaps: float32 [3], replicated
- pruned_counts: float32 [2], replicated
The draws below stay inside these ranges and needn't reach their ends.
All inputs are finite; a program needn't handle non-finite values. No bound on the sum of `active_mask` on one device may be relied on, other than what follows from the above.
Results may differ from the reference program's by a relative error of at most 0.0024.
The reference program's roundings to bfloat16 on the way count: a program that leaves them out, or rounds other values in their place, can miss the bound.
Values may be sent and summed in bfloat16 or wider, within the bound.
A program may use at most 64 MiB of HBM per device.

```python
import jax
import jax.numpy as jnp
from jax import lax

K = 128
ITERS = 2
NS = 14336
P_SIZE = 65536


def draw_targets(key, part):
    phase_key = jax.random.fold_in(key, 11)
    rough_key = jax.random.fold_in(key, 12)
    noise_key = jax.random.fold_in(key, 13)
    positions = jnp.arange(NS).astype(jnp.float32) / NS
    phase = jax.random.uniform(phase_key, (), jnp.float32, 0.0, 6.2831853)
    profile = jnp.exp(1.5 * jnp.sin(6.2831853 * 3.0 * positions + phase))
    rough = jax.random.uniform(rough_key, (NS, 1), jnp.float32, 0.7, 1.4)
    noise = jnp.clip(jax.random.normal(noise_key, (NS, K), jnp.float32), -4.0, 4.0)
    return (noise * profile[:, None] * rough).astype(jnp.bfloat16)


def plant(drawn, key, smallest, top_value):
    extent = drawn.shape
    index_at = [jax.random.randint(jax.random.fold_in(key, axis), (), 0, extent[axis]) for axis in range(len(extent))]
    drawn = drawn.at[tuple(index_at)].set(smallest)
    longest = extent.index(max(extent))
    index_at[longest] = (index_at[longest] + 1) % extent[longest]
    return drawn.at[tuple(index_at)].set(top_value)


def with_spikes(values, own_key, source, target, parts, factor):
    owner, partner = [(jnp.arange(values.shape[axis_at]) // (values.shape[axis_at] // parts)).reshape([-1 if axis == axis_at else 1 for axis in range(values.ndim)]) for axis_at in (source, target)]
    chosen = jax.random.permutation(own_key, parts)[partner]
    strong = (owner == chosen) | (owner == (partner + parts // 2) % parts)
    return jnp.where(strong, factor * values, values)


def levels(rng, extent, pieces, least, high):
    loudness, own = 1.0, jax.random.fold_in(rng, 6)
    for dim, blocks in pieces:
        steps = jnp.exp(jax.random.uniform(jax.random.fold_in(own, dim), (blocks,), jnp.float32, least / len(pieces), high / len(pieces)))
        loudness = loudness * jnp.repeat(steps, extent[dim] // blocks).reshape([-1 if axis == dim else 1 for axis in range(len(extent))])
    return loudness


def scatter_about(stream_key, extent, scale, reach, cuts=(), held_as=jnp.bfloat16):
    drawn = jax.random.normal(stream_key, extent, jnp.float32) * scale
    if len(cuts) > 0:
        drawn = levels(stream_key, extent, cuts, -0.22, 0.18) * drawn
    return jnp.clip(drawn, min=-reach, max=reach).astype(held_as)


def gaussian_with(stream_key, shape, spread, bound, shards, heavy, kind=jnp.bfloat16):
    result = spread * jax.random.normal(stream_key, shape, jnp.float32)
    if shards:
        result = result * levels(stream_key, shape, shards, -0.22, 0.18)
    return jnp.clip(with_spikes(result, jax.random.fold_in(stream_key, 3), *heavy), -bound, bound).astype(kind)


def setup_inputs(seed: int = 0) -> dict:
    key_list = jax.random.split(jax.random.key(seed), 6)
    design = gaussian_with(key_list[0], (NS, P_SIZE), NS ** -0.5, 0.125, ((0, 4), (1, 64)), (1, 0, 64, 4.0))
    targets = draw_targets(jax.random.fold_in(key_list[5], 71), 0)
    warm_start = scatter_about(key_list[2], (P_SIZE, K), 0.1, 0.6, ((0, 64),), jnp.float32)
    active_mask = plant((jax.random.randint(key_list[3], (ITERS, P_SIZE), 0, 4) < 3).astype(jnp.int32), jax.random.fold_in(key_list[3], 1), 0, 1)
    penalty_index = jax.random.randint(key_list[4], (1,), 0, 8).astype(jnp.int32)
    return {"design": design, "targets": targets, "warm_start": warm_start, "active_mask": active_mask, "penalty_index": penalty_index}


def group_norms(matrix):
    return jnp.sqrt(lax.optimization_barrier(jnp.sum(matrix * matrix, axis=1)))

def transpose_product(design, right_side):
    return lax.dot_general(design, right_side, (((0,), (0,)), ((), ())), preferred_element_type=jnp.float32)

def reference(design, targets, warm_start, active_mask, penalty_index):
    corr_y = transpose_product(design, targets)
    column_squares = lax.optimization_barrier(jnp.sum(jnp.square(design.astype(jnp.float32)), axis=0))
    penalty_max = jnp.max(group_norms(corr_y))
    penalty = penalty_max / (8.0 + 4.0 * penalty_index[0].astype(jnp.float32))
    step_sizes = 0.5 / (1.0 + column_squares)
    target_float = targets.astype(jnp.float32)
    current = warm_start
    correlations = []
    relative_gaps = []
    pruned_counts = []
    for iteration in range(ITERS + 1):
        current_half = current.astype(jnp.bfloat16)
        fitted = jnp.dot(design, current_half, preferred_element_type=jnp.float32)
        residual = (target_float - fitted).astype(jnp.bfloat16)
        resid_float = residual.astype(jnp.float32)
        rr_sum = jnp.sum(resid_float * resid_float)
        ry_sum = jnp.sum(resid_float * target_float)
        bn_sum = jnp.sum(group_norms(current))
        gradient = transpose_product(design, residual)
        grad_norms = group_norms(gradient)
        scale = jnp.maximum(penalty, jnp.max(grad_norms))
        correlations.append(grad_norms / scale)
        primal = 0.5 * rr_sum + penalty * bn_sum
        ratio = penalty / scale
        dual = ratio * ry_sum - 0.5 * ratio * ratio * rr_sum
        relative_gaps.append((primal - dual) / (primal + 1.0))
        if iteration < ITERS:
            keep = active_mask[iteration].astype(jnp.float32)
            pruned_counts.append(jnp.sum(1.0 - keep))
            moved = current + step_sizes[:, None] * gradient
            moved_norms = group_norms(moved)
            cutoff = step_sizes * penalty
            factor = jnp.maximum(moved_norms - cutoff, 0.0) / jnp.maximum(moved_norms, cutoff)
            current = (keep * factor)[:, None] * moved
    return (current, jnp.stack(correlations), jnp.stack(relative_gaps), jnp.stack(pruned_counts))
```

```python
import jax
import jax.numpy as jnp
from jax import lax
from jax.experimental import pallas as pl
from jax.experimental.pallas import tpu as pltpu
from jax.sharding import Mesh
from jax.sharding import PartitionSpec as P

ITERS = 2
NY, NZ, NX = 4, 8, 4
MESH = pl.DeviceIdType.MESH
F32 = jnp.float32
BF16 = jnp.bfloat16
Y_TYPES = (BF16, F32, BF16)
Z_TYPES = (BF16, F32, BF16)
X_TYPES = (F32, F32, BF16, BF16)


def lanes_folded(row, op):
    return op(row[:, :128], row[:, 128:])


def column_norms(matrix):
    return jnp.sqrt(jnp.sum(matrix * matrix, axis=0, keepdims=True))


def kernel(
    design, targets, target_blocks, warm, mask, penalty_index,
    coef, corr, gaps, counts,
    D, T, own_targets, half, cs, cr, ys, yr, keep, zt, zs, zr, R, G, gs, gr,
    current, coef_parts, cqs, cqr, pen_src, pen_z, pen_y, pen_c, pen_x,
    norms, fin_src, fin_x, fin_c, fin_y, fin_z, stats, load_sem, send_sem, recv_sem,
):
    y, z, c, x = (lax.axis_index(a) for a in ("y", "z", "c", "x"))
    oc = 1 - c
    step = 1 - 2 * c
    yf, yb, y2 = lax.rem(y + step + NY, NY), lax.rem(y - step + NY, NY), lax.rem(y + 2, NY)
    xf, xb, x2 = lax.rem(x + step + NX, NX), lax.rem(x - step + NX, NX), lax.rem(x + 2, NX)
    block = D.shape[0] // (2 * NY)
    quarter = D.shape[1] // NX
    sub = block // NZ
    task_count = warm.shape[1]

    def rows(cc, yy):
        return pl.ds(pl.multiple_of((cc * NY + yy) * block, block), block)

    def cols(xx):
        return pl.ds(pl.multiple_of(xx * quarter, quarter), quarter)

    used = [0]
    pending = []

    def send(src, dst, device):
        i = used[0]
        used[0] += 1
        copy = pltpu.make_async_remote_copy(
            src_ref=src, dst_ref=dst, send_sem=send_sem.at[i], recv_sem=recv_sem.at[i],
            device_id=device, device_id_type=MESH,
        )
        copy.start()
        pending.append(copy)
        return copy

    def drain():
        for copy in pending:
            copy.wait_send()
        pending.clear()

    def to_all(src, dst, axis, me, n):
        return [
            send(src, dst.at[d - 1], {axis: lax.rem(me + d, n)}) for d in range(1, n)
        ]

    def waited(copies):
        for copy in copies:
            copy.wait_recv()

    others, mine = (y2, yf, yb, y), (y2, yb, yf, y)
    steps = (("o", 0), ("o", 1), ("m", 0), ("o", 2), ("m", 1), ("o", 3), ("m", 2), ("m", 3))
    loads = {}
    for i, (kind, j) in enumerate(steps):
        cc, yy = (oc, others[j]) if kind == "o" else (c, mine[j])
        load = pltpu.make_async_copy(design.at[rows(cc, yy), :], D.at[rows(cc, yy), :], load_sem.at[i])
        load.start()
        loads[kind, j] = load
    own_load = pltpu.make_async_copy(
        target_blocks.at[(c * NY + y) * NZ + z], own_targets, load_sem.at[8]
    )
    own_load.start()
    target_load = pltpu.make_async_copy(targets, T, load_sem.at[9])
    target_load.start()

    barrier = pltpu.get_barrier_semaphore()
    peers = (
        [{"c": oc}]
        + [{"y": lax.rem(y + d, NY)} for d in range(1, NY)]
        + [{"z": lax.rem(z + d, NZ)} for d in range(1, NZ)]
        + [{"x": lax.rem(x + d, NX)} for d in range(1, NX)]
    )
    for peer in peers:
        pl.semaphore_signal(barrier, inc=1, device_id=peer, device_id_type=MESH)

    half[0] = warm[...].astype(BF16).reshape(half.shape[1:])
    current[...] = warm[cols(x), :].T
    bn = [column_norms(current[...])]
    pl.semaphore_wait(barrier, len(peers))

    def grad_block(R_t, cc, yy, first):
        part = R_t[cc, yy].astype(F32).reshape(block, task_count).astype(BF16)
        product = lax.dot_general(
            part, D[rows(cc, yy), :], (((0,), (0,)), ((), ())), preferred_element_type=F32
        )
        if first:
            G[...] = product
        else:
            G[...] += product

    def ring_start(k):
        gs[k][0] = G[:, cols(x2)].astype(X_TYPES[k])
        a = send(gs[k].at[0], gr[k].at[0], {"x": xf})
        gs[k][1] = G[:, cols(xb)].astype(X_TYPES[k])
        b = send(gs[k].at[1], gr[k].at[1], {"x": xb})
        return a, b

    def ring_middle(k, a):
        a.wait_recv()
        gs[k][2] = (G[:, cols(xf)] + gr[k][0].astype(F32)).astype(X_TYPES[k])
        return send(gs[k].at[2], gr[k].at[2], {"x": xf})

    def ring_end(k, b, last):
        b.wait_recv()
        last.wait_recv()
        return G[:, cols(x)] + gr[k][1].astype(F32) + gr[k][2].astype(F32)

    def maximum_of(src, arrived):
        value = src
        for d in range(arrived.shape[0]):
            value = jnp.maximum(value, arrived[d])
        return value

    penalty = step_sizes = None
    coef_copies = []
    rr, ry, pruned = [], [], []
    for t in range(ITERS + 1):
        weights = half[t].reshape(D.shape[1], task_count)

        def product(cc, yy):
            return jnp.dot(D[rows(cc, yy), :], weights, preferred_element_type=F32)

        core_copies = []

        def other(j):
            if t == 0:
                loads["o", j].wait()
            cs[j] = product(oc, others[j])
            core_copies.append(send(cs.at[j], cr.at[t, j], {"c": oc}))

        def summed(j):
            if t == 0:
                loads["m", j].wait()
            own = product(c, mine[j])
            core_copies[j].wait_recv()
            return own + cr[t, j]

        other(0)
        other(1)
        ys[t][0] = summed(0).astype(Y_TYPES[t])
        ya = send(ys[t].at[0], yr[t].at[0], {"y": yf})
        other(2)
        ys[t][1] = summed(1).astype(Y_TYPES[t])
        yb_copy = send(ys[t].at[1], yr[t].at[1], {"y": yb})
        other(3)
        keep[0] = summed(2)
        keep[1] = summed(3)
        if t == 0:
            target_load.wait()
            for b in range(2 * NY):
                part = T[b * block : (b + 1) * block, :]
                corr_product = lax.dot_general(
                    part, D[b * block : (b + 1) * block, :], (((0,), (0,)), ((), ())),
                    preferred_element_type=F32,
                )
                if b == 0:
                    G[...] = corr_product
                else:
                    G[...] += corr_product
            ca, cb = ring_start(ITERS + 1)
        ya.wait_recv()
        ys[t][2] = (keep[0] + yr[t][0].astype(F32)).astype(Y_TYPES[t])
        yc = send(ys[t].at[2], yr[t].at[2], {"y": yf})
        if t == 0:
            def square_step(i, total):
                v = D[pl.ds(pl.multiple_of(i * 64, 64), 64), :].astype(F32)
                return total + jnp.sum((v * v).reshape(8, 8, v.shape[1]), axis=0)

            squares = lax.fori_loop(
                0, D.shape[0] // 64, square_step, jnp.zeros((8, D.shape[1]), F32)
            )
            squares = jnp.sum(squares, axis=0, keepdims=True)
            for q in range(NX):
                cqs[q] = jnp.broadcast_to(squares[:, q * quarter : (q + 1) * quarter], (8, quarter))
            square_copies = [
                send(cqs.at[lax.rem(x + d, NX)], cqr.at[d - 1], {"x": lax.rem(x + d, NX)})
                for d in range(1, NX)
            ]
            cc_copy = ring_middle(ITERS + 1, ca)
        yb_copy.wait_recv()
        yc.wait_recv()
        total = (keep[1] + yr[t][1].astype(F32) + yr[t][2].astype(F32)).reshape(NZ, sub, task_count)
        zt[...] = total
        zs[t][...] = total.astype(Z_TYPES[t])
        z_copies = []
        for d in range(1, NZ):
            zz = lax.rem(z + d, NZ)
            z_copies.append(send(zs[t].at[zz], zr[t].at[d - 1], {"z": zz}))
        if t == 0:
            corr_y = ring_end(ITERS + 1, cb, cc_copy)
            top = lanes_folded(column_norms(corr_y), jnp.maximum)
            pen_src[0] = jnp.broadcast_to(top, (8, 128))
            pen_copies = to_all(pen_src.at[0], pen_z, "z", z, NZ)
            own_load.wait()
        waited(z_copies)
        fitted = zt[z]
        for d in range(NZ - 1):
            fitted = fitted + zr[t][d].astype(F32)
        target_float = own_targets[...].astype(F32)
        residual = (target_float - fitted).astype(BF16)
        R[t, c, y, z] = residual
        own_rows = R.at[t, c, y, z]
        r_copies = [send(own_rows, own_rows, {"z": lax.rem(z + d, NZ)}) for d in range(1, NZ)]
        resid_float = residual.astype(F32)
        rr.append(jnp.sum(resid_float * resid_float, axis=0, keepdims=True))
        ry.append(jnp.sum(resid_float * target_float, axis=0, keepdims=True))
        if t == 0:
            waited(pen_copies)
            pen_src[1] = maximum_of(pen_src[0], pen_z)
            pen_copies = to_all(pen_src.at[1], pen_y, "y", y, NY)
        waited(r_copies)

        def block_to(yy, device):
            return send(R.at[t, c, yy], R.at[t, c, yy], device)

        R_t = R.at[t]
        g1 = block_to(y, {"y": yf})
        g2 = block_to(y, {"y": yb})
        q0 = block_to(y, {"c": oc})
        if t == 0:
            waited(pen_copies)
            pen_src[2] = maximum_of(pen_src[1], pen_y)
            pen_copies = to_all(pen_src.at[2], pen_c, "c", c, 2)
        grad_block(R_t, c, y, True)
        q0.wait_recv()
        grad_block(R_t, oc, y, False)
        g1.wait_recv()
        g3 = block_to(yb, {"y": yf})
        q1 = block_to(yb, {"c": oc})
        g2.wait_recv()
        q2 = block_to(yf, {"c": oc})
        if t == 0:
            waited(pen_copies)
            pen_src[3] = maximum_of(pen_src[2], pen_c)
            pen_copies = to_all(pen_src.at[3], pen_x, "x", x, NX)
        grad_block(R_t, c, yb, False)
        grad_block(R_t, c, yf, False)
        q1.wait_recv()
        grad_block(R_t, oc, yf, False)
        g3.wait_recv()
        q3 = block_to(y2, {"c": oc})
        q2.wait_recv()
        grad_block(R_t, oc, yb, False)
        grad_block(R_t, c, y2, False)
        q3.wait_recv()
        grad_block(R_t, oc, y2, False)
        ga, gb = ring_start(t)
        if t == 0:
            waited(pen_copies)
            pen_max = jnp.max(maximum_of(pen_src[3], pen_x), axis=(0, 1), keepdims=True)
            penalty = pen_max / (8.0 + 4.0 * penalty_index[0].astype(F32))
            waited(square_copies)
            total_squares = (cqs[x] + cqr[0] + cqr[1] + cqr[2])[0:1, :]
            step_sizes = 0.5 / (1.0 + total_squares)
        gc = ring_middle(t, ga)
        gradient = ring_end(t, gb, gc)
        drain()
        grad_norms = column_norms(gradient)
        norms[x, t : t + 1, :] = grad_norms
        stats[16 + t : 17 + t, :] = lanes_folded(grad_norms, jnp.maximum)
        if t < ITERS:
            active = mask[t : t + 1, cols(x)].astype(F32)
            pruned.append(1.0 - active)
            moved = current[...] + step_sizes * gradient
            moved_norms = column_norms(moved)
            cutoff = step_sizes * penalty
            factor = jnp.maximum(moved_norms - cutoff, 0.0) / jnp.maximum(moved_norms, cutoff)
            updated = (active * factor) * moved
            flipped = updated.T
            half[t + 1, x] = flipped.astype(BF16)
            own_half = half.at[t + 1, x]
            h1 = send(own_half, own_half, {"x": xf})
            h2 = send(own_half, own_half, {"x": xb})
            current[...] = updated
            bn.append(column_norms(updated))
            if t == ITERS - 1:
                coef_parts[x] = flipped
            h1.wait_recv()
            h3 = send(half.at[t + 1, xb], half.at[t + 1, xb], {"x": xf})
            h2.wait_recv()
            h3.wait_recv()
            if t == ITERS - 1:
                own_coef = coef_parts.at[x]
                coef_copies = [send(own_coef, own_coef, {"x": xq}) for xq in (xf, xb, x2)]

    for i, value in enumerate(rr + ry):
        stats[i : i + 1, :] = value
    for i, value in enumerate(bn + pruned):
        stats[6 + i : 7 + i, :] = lanes_folded(value, jnp.add)
    stats[11:16, :] = jnp.zeros((5, 128), F32)
    stats[19:24, :] = jnp.zeros((5, 128), F32)
    norms[x, 3:8, :] = jnp.zeros((5, quarter), F32)
    own_norms = norms.at[x]
    norm_copies = [send(own_norms, own_norms, {"x": xq}) for xq in (xf, xb, x2)]
    fin_src[0] = stats[...]
    for k, (arrived, axis, me, n) in enumerate(
        ((fin_x, "x", x, NX), (fin_c, "c", c, 2), (fin_y, "y", y, NY), (fin_z, "z", z, NZ))
    ):
        copies = to_all(fin_src.at[k], arrived, axis, me, n)
        if k == 1:
            waited(coef_copies)
            for q in range(NX):
                coef[q * quarter : (q + 1) * quarter, :] = coef_parts[q]
        waited(copies)
        sums, tops = fin_src[k, 0:16, :], fin_src[k, 16:24, :]
        for d in range(n - 1):
            sums = sums + arrived[d, 0:16, :]
            tops = jnp.maximum(tops, arrived[d, 16:24, :])
        if k < 3:
            fin_src[k + 1, 0:16, :] = sums
            fin_src[k + 1, 16:24, :] = tops
    sums = jnp.sum(sums, axis=1, keepdims=True)
    tops = jnp.max(tops, axis=1, keepdims=True)
    waited(norm_copies)
    for t in range(ITERS + 1):
        scale = jnp.maximum(penalty, tops[t : t + 1, :])
        for q in range(NX):
            corr[t : t + 1, q * quarter : (q + 1) * quarter] = norms[q, t : t + 1, :] / scale
        rr_sum, ry_sum, bn_sum = sums[t : t + 1], sums[3 + t : 4 + t], sums[6 + t : 7 + t]
        primal = 0.5 * rr_sum + penalty * bn_sum
        ratio = penalty / scale
        dual = ratio * ry_sum - 0.5 * ratio * ratio * rr_sum
        gaps[t] = jnp.sum((primal - dual) / (primal + 1.0))
    for t in range(ITERS):
        counts[t] = jnp.sum(sums[9 + t : 10 + t])
    drain()
    assert used[0] == send_sem.shape[0], used[0]


def local(design, targets, warm_start, active_mask, penalty_index):
    samples, features = design.shape
    tasks = targets.shape[1]
    block = samples // (2 * NY)
    sub = block // NZ
    quarter = features // NX
    steps = ITERS + 1
    vmem, smem, hbm = pltpu.VMEM, pltpu.SMEM, pl.ANY
    target_blocks = targets.reshape(2 * NY * NZ, sub, tasks)
    scratch = [
        vmem((samples, features), BF16),
        vmem((samples, tasks), BF16),
        vmem((sub, tasks), BF16),
        vmem((steps, NX, quarter, tasks), BF16),
        vmem((4, block, tasks), F32),
        vmem((steps, 4, block, tasks), F32),
        tuple(vmem((3, block, tasks), v) for v in Y_TYPES),
        tuple(vmem((3, block, tasks), v) for v in Y_TYPES),
        vmem((2, block, tasks), F32),
        vmem((NZ, sub, tasks), F32),
        tuple(vmem((NZ, sub, tasks), v) for v in Z_TYPES),
        tuple(vmem((NZ - 1, sub, tasks), v) for v in Z_TYPES),
        vmem((steps, 2, NY, NZ, sub, tasks), BF16),
        vmem((tasks, features), F32),
        tuple(vmem((3, tasks, quarter), v) for v in X_TYPES),
        tuple(vmem((3, tasks, quarter), v) for v in X_TYPES),
        vmem((tasks, quarter), F32),
        vmem((NX, quarter, tasks), F32),
        vmem((NX, 8, quarter), F32),
        vmem((NX - 1, 8, quarter), F32),
        vmem((4, 8, 128), F32),
        vmem((NZ - 1, 8, 128), F32),
        vmem((NY - 1, 8, 128), F32),
        vmem((1, 8, 128), F32),
        vmem((NX - 1, 8, 128), F32),
        vmem((NX, 8, quarter), F32),
        vmem((4, 24, 128), F32),
        vmem((NX - 1, 24, 128), F32),
        vmem((1, 24, 128), F32),
        vmem((NY - 1, 24, 128), F32),
        vmem((NZ - 1, 24, 128), F32),
        vmem((24, 128), F32),
        pltpu.SemaphoreType.DMA((10,)),
        pltpu.SemaphoreType.DMA((139,)),
        pltpu.SemaphoreType.DMA((139,)),
    ]
    return pl.pallas_call(
        kernel,
        out_shape=(
            jax.ShapeDtypeStruct((features, tasks), F32),
            jax.ShapeDtypeStruct((steps, features), F32),
            jax.ShapeDtypeStruct((steps,), F32),
            jax.ShapeDtypeStruct((ITERS,), F32),
        ),
        in_specs=[
            pl.BlockSpec(memory_space=hbm),
            pl.BlockSpec(memory_space=hbm),
            pl.BlockSpec(memory_space=hbm),
            pl.BlockSpec(memory_space=vmem),
            pl.BlockSpec(memory_space=vmem),
            pl.BlockSpec(memory_space=smem),
        ],
        out_specs=(
            pl.BlockSpec(memory_space=vmem),
            pl.BlockSpec(memory_space=vmem),
            pl.BlockSpec(memory_space=smem),
            pl.BlockSpec(memory_space=smem),
        ),
        scratch_shapes=scratch,
        compiler_params=pltpu.CompilerParams(
            collective_id=0, has_side_effects=True, vmem_limit_bytes=60 * 1024 * 1024
        ),
        name="lasso_steps",
    )(design, targets, target_blocks, warm_start, active_mask, penalty_index)


def solution(mesh):
    torus = Mesh(mesh.devices.reshape(NY, NZ, 2, NX), ("y", "z", "c", "x"))
    feat = ("y", "z", "c")
    in_specs = (P("x", feat), P("x", None), P(feat, None), P(None, feat), P())
    out_specs = (P(feat, None), P(None, feat), P(), P())
    return jax.shard_map(local, mesh=torus, in_specs=in_specs, out_specs=out_specs, check_vma=False)
```

```python
import jax
import jax.numpy as jnp
from jax import lax
from jax.experimental import pallas as pl
from jax.experimental.pallas import tpu as pltpu
from jax.sharding import Mesh
from jax.sharding import PartitionSpec as P

ITERS = 2
NY, NZ, NX = 4, 8, 4
MESH = pl.DeviceIdType.MESH
FAR_FIRST = (4, 3, 5, 2, 6, 1, 7)
F32 = jnp.float32
BF16 = jnp.bfloat16
Y_TYPES = (BF16, F32, BF16)
Z_TYPES = (BF16, F32, BF16)
X_TYPES = (F32, F32, BF16, BF16)


def lanes_folded(row, op):
    return op(row[:, :128], row[:, 128:])


def column_norms(matrix):
    return jnp.sqrt(jnp.sum(matrix * matrix, axis=0, keepdims=True))


def kernel(
    design, targets, target_blocks, warm, mask, penalty_index,
    coef, corr, gaps, counts,
    D, T, own_targets, half, cs, cr, ys, yr, keep, zt, zs, zr, R, G, gs, gr,
    current, coef_parts, cqs, cqr, pen_src, pen_z, pen_y, pen_c, pen_x,
    norms, fin_src, fin_plane, fin_column, stats, load_sem, send_sem, recv_sem,
):
    y, z, c, x = (lax.axis_index(a) for a in ("y", "z", "c", "x"))
    oc = 1 - c
    step = 1 - 2 * c
    yf, yb, y2 = lax.rem(y + step + NY, NY), lax.rem(y - step + NY, NY), lax.rem(y + 2, NY)
    xf, xb, x2 = lax.rem(x + step + NX, NX), lax.rem(x - step + NX, NX), lax.rem(x + 2, NX)
    block = D.shape[0] // (2 * NY)
    quarter = D.shape[1] // NX
    sub = block // NZ
    task_count = warm.shape[1]

    def rows(cc, yy):
        return pl.ds(pl.multiple_of((cc * NY + yy) * block, block), block)

    def cols(xx):
        return pl.ds(pl.multiple_of(xx * quarter, quarter), quarter)

    used = [0]
    pending = []

    def send(src, dst, device):
        i = used[0]
        used[0] += 1
        copy = pltpu.make_async_remote_copy(
            src_ref=src, dst_ref=dst, send_sem=send_sem.at[i], recv_sem=recv_sem.at[i],
            device_id=device, device_id_type=MESH,
        )
        copy.start()
        pending.append(copy)
        return copy

    def drain():
        for copy in pending:
            copy.wait_send()
        pending.clear()

    def to_all(src, dst, axis, me, n):
        return [
            send(src, dst.at[d - 1], {axis: lax.rem(me + d, n)}) for d in range(1, n)
        ]

    def waited(copies):
        for copy in copies:
            copy.wait_recv()

    others, mine = (y2, yf, yb, y), (y2, yb, yf, y)
    steps = (("o", 0), ("o", 1), ("m", 0), ("o", 2), ("m", 1), ("o", 3), ("m", 2), ("m", 3))
    loads = {}
    for i, (kind, j) in enumerate(steps):
        cc, yy = (oc, others[j]) if kind == "o" else (c, mine[j])
        load = pltpu.make_async_copy(design.at[rows(cc, yy), :], D.at[rows(cc, yy), :], load_sem.at[i])
        load.start()
        loads[kind, j] = load
    own_load = pltpu.make_async_copy(
        target_blocks.at[(c * NY + y) * NZ + z], own_targets, load_sem.at[8]
    )
    own_load.start()
    target_load = pltpu.make_async_copy(targets, T, load_sem.at[9])
    target_load.start()

    barrier = pltpu.get_barrier_semaphore()
    peers = (
        [{"c": oc}]
        + [{"y": lax.rem(y + d, NY)} for d in range(1, NY)]
        + [{"z": lax.rem(z + d, NZ)} for d in range(1, NZ)]
        + [{"x": lax.rem(x + d, NX)} for d in range(1, NX)]
    )
    plane = [
        {"x": lax.rem(x + d, NX), "y": lax.rem(y + e, NY)}
        for d in range(NX) for e in range(NY) if d or e
    ]
    column = [
        {"z": lax.rem(z + d, NZ), "c": lax.rem(c + e, 2)} for d in range(NZ) for e in range(2) if d or e
    ]
    peers += [
        {"x": lax.rem(x + d, NX), "y": lax.rem(y + e, NY)} for d in range(1, NX) for e in range(1, NY)
    ]
    peers += [{"z": lax.rem(z + d, NZ), "c": oc} for d in range(1, NZ)]
    for peer in peers:
        pl.semaphore_signal(barrier, inc=1, device_id=peer, device_id_type=MESH)

    half[0] = warm[...].astype(BF16).reshape(half.shape[1:])
    current[...] = warm[cols(x), :].T
    bn = [column_norms(current[...])]

    def grad_block(R_t, cc, yy, first):
        part = R_t[cc, yy].astype(F32).reshape(block, task_count).astype(BF16)
        product = lax.dot_general(
            part, D[rows(cc, yy), :], (((0,), (0,)), ((), ())), preferred_element_type=F32
        )
        if first:
            G[...] = product
        else:
            G[...] += product

    task_halves = [pl.ds(h * task_count // 2, task_count // 2) for h in range(2)]

    def ring_start(k):
        gs[k][0] = G[:, cols(x2)].astype(X_TYPES[k])
        a = [send(gs[k].at[0, p], gr[k].at[0, p], {"x": xf}) for p in task_halves]
        gs[k][1] = G[:, cols(xb)].astype(X_TYPES[k])
        b = send(gs[k].at[1], gr[k].at[1], {"x": xb})
        return a, b

    def ring_middle(k, a):
        last = []
        for copy, p in zip(a, task_halves):
            copy.wait_recv()
            gs[k][2, p, :] = (G[p, cols(xf)] + gr[k][0, p, :].astype(F32)).astype(X_TYPES[k])
            last.append(send(gs[k].at[2, p], gr[k].at[2, p], {"x": xf}))
        return last

    def ring_end(k, b, last):
        b.wait_recv()
        waited(last)
        return G[:, cols(x)] + gr[k][1].astype(F32) + gr[k][2].astype(F32)

    def maximum_of(src, arrived):
        value = src
        for d in range(arrived.shape[0]):
            value = jnp.maximum(value, arrived[d])
        return value

    penalty = step_sizes = None
    coef_copies = []
    rr, ry, pruned = [], [], []
    for t in range(ITERS + 1):
        weights = half[t].reshape(D.shape[1], task_count).astype(F32).T.astype(BF16)

        def product(cc, yy):
            turned = lax.dot_general(
                weights, D[rows(cc, yy), :], (((1,), (1,)), ((), ())), preferred_element_type=F32
            )
            return turned.T

        core_copies = []

        def halved(src, dst, device, length):
            parts = [pl.ds(h * length // 2, length // 2) for h in range(2)]
            return [send(src.at[p], dst.at[p], device) for p in parts]

        def other(j):
            if t == 0:
                loads["o", j].wait()
            cs[j] = product(oc, others[j])
            if t == 0 and j == 0:
                pl.semaphore_wait(barrier, len(peers))
            core_copies.append(send(cs.at[j], cr.at[t, j], {"c": oc}))

        def summed(j):
            if t == 0:
                loads["m", j].wait()
            own = product(c, mine[j])
            core_copies[j].wait_recv()
            return own + cr[t, j]

        other(0)
        other(1)
        ys[t][0] = summed(0).astype(Y_TYPES[t])
        ya = halved(ys[t].at[0], yr[t].at[0], {"y": yf}, block)
        other(2)
        ys[t][1] = summed(1).astype(Y_TYPES[t])
        yb_copy = send(ys[t].at[1], yr[t].at[1], {"y": yb})
        other(3)
        keep[0] = summed(2)
        keep[1] = summed(3)
        if t == 0:
            target_load.wait()
            for b in range(2 * NY):
                part = T[b * block : (b + 1) * block, :]
                corr_product = lax.dot_general(
                    part, D[b * block : (b + 1) * block, :], (((0,), (0,)), ((), ())),
                    preferred_element_type=F32,
                )
                if b == 0:
                    G[...] = corr_product
                else:
                    G[...] += corr_product
            ca, cb = ring_start(ITERS + 1)
        yc = []
        for h in range(2):
            ya[h].wait_recv()
            p = pl.ds(h * block // 2, block // 2)
            ys[t][2, p, :] = (keep[0, p, :] + yr[t][0, p, :].astype(F32)).astype(Y_TYPES[t])
            yc.append(send(ys[t].at[2, p], yr[t].at[2, p], {"y": yf}))
        if t == 0:
            def square_step(i, total):
                v = D[pl.ds(pl.multiple_of(i * 64, 64), 64), :].astype(F32)
                return total + jnp.sum((v * v).reshape(8, 8, v.shape[1]), axis=0)

            squares = lax.fori_loop(
                0, D.shape[0] // 64, square_step, jnp.zeros((8, D.shape[1]), F32)
            )
            squares = jnp.sum(squares, axis=0, keepdims=True)
            for q in range(NX):
                cqs[q] = jnp.broadcast_to(squares[:, q * quarter : (q + 1) * quarter], (8, quarter))
            square_copies = [
                send(cqs.at[lax.rem(x + d, NX)], cqr.at[d - 1], {"x": lax.rem(x + d, NX)})
                for d in range(1, NX)
            ]
            cc_copy = ring_middle(ITERS + 1, ca)
        yb_copy.wait_recv()
        waited(yc)
        total = (keep[1] + yr[t][1].astype(F32) + yr[t][2].astype(F32)).reshape(NZ, sub, task_count)
        zt[...] = total
        zs[t][...] = total.astype(Z_TYPES[t])
        z_copies = []
        for d in FAR_FIRST:
            zz = lax.rem(z + d, NZ)
            z_copies.append(send(zs[t].at[zz], zr[t].at[d - 1], {"z": zz}))
        if t == 0:
            corr_y = ring_end(ITERS + 1, cb, cc_copy)
            top = lanes_folded(column_norms(corr_y), jnp.maximum)
            pen_src[0] = jnp.broadcast_to(top, (8, 128))
            pen_copies = to_all(pen_src.at[0], pen_z, "z", z, NZ)
            own_load.wait()
        waited(z_copies)
        fitted = zt[z]
        for d in range(NZ - 1):
            fitted = fitted + zr[t][d].astype(F32)
        target_float = own_targets[...].astype(F32)
        residual = (target_float - fitted).astype(BF16)
        R[t, c, y, z] = residual
        own_rows = R.at[t, c, y, z]
        r_copies = [send(own_rows, own_rows, {"z": lax.rem(z + d, NZ)}) for d in FAR_FIRST]
        resid_float = residual.astype(F32)
        rr.append(jnp.sum(resid_float * resid_float, axis=0, keepdims=True))
        ry.append(jnp.sum(resid_float * target_float, axis=0, keepdims=True))
        near_first = (0, *reversed(FAR_FIRST))
        g1, g2 = [], []
        for d in near_first:
            if d:
                r_copies[FAR_FIRST.index(d)].wait_recv()
            through = R.at[t, c, y, lax.rem(z - d + NZ, NZ)]
            g1.append(send(through, through, {"y": yf}))
            g2.append(send(through, through, {"y": yb}))

        def block_to(yy, device):
            return send(R.at[t, c, yy], R.at[t, c, yy], device)

        R_t = R.at[t]
        q0 = block_to(y, {"c": oc})
        if t == 0:
            waited(pen_copies)
            pen_src[1] = maximum_of(pen_src[0], pen_z)
            pen_copies = to_all(pen_src.at[1], pen_y, "y", y, NY)
        grad_block(R_t, c, y, True)
        q0.wait_recv()
        grad_block(R_t, oc, y, False)
        g3 = []
        for d, copy in zip(near_first, g1):
            copy.wait_recv()
            through = R.at[t, c, yb, lax.rem(z - d + NZ, NZ)]
            g3.append(send(through, through, {"y": yf}))
        q1 = block_to(yb, {"c": oc})
        waited(g2)
        q2 = block_to(yf, {"c": oc})
        if t == 0:
            waited(pen_copies)
            pen_src[2] = maximum_of(pen_src[1], pen_y)
            pen_copies = to_all(pen_src.at[2], pen_c, "c", c, 2)
        grad_block(R_t, c, yb, False)
        grad_block(R_t, c, yf, False)
        q1.wait_recv()
        grad_block(R_t, oc, yf, False)
        q3 = []
        for d, copy in zip(near_first, g3):
            copy.wait_recv()
            through = R.at[t, c, y2, lax.rem(z - d + NZ, NZ)]
            q3.append(send(through, through, {"c": oc}))
        q2.wait_recv()
        grad_block(R_t, oc, yb, False)
        grad_block(R_t, c, y2, False)
        waited(q3)
        grad_block(R_t, oc, y2, False)
        ga, gb = ring_start(t)
        if t == 0:
            waited(pen_copies)
            pen_src[3] = maximum_of(pen_src[2], pen_c)
            pen_copies = to_all(pen_src.at[3], pen_x, "x", x, NX)
        gc = ring_middle(t, ga)
        if t == 0:
            waited(pen_copies)
            pen_max = jnp.max(maximum_of(pen_src[3], pen_x), axis=(0, 1), keepdims=True)
            penalty = pen_max / (8.0 + 4.0 * penalty_index[0].astype(F32))
            waited(square_copies)
            total_squares = (cqs[x] + cqr[0] + cqr[1] + cqr[2])[0:1, :]
            step_sizes = 0.5 / (1.0 + total_squares)
        gradient = ring_end(t, gb, gc)
        drain()
        grad_norms = column_norms(gradient)
        norms[x, t : t + 1, :] = grad_norms
        stats[16 + t : 17 + t, :] = lanes_folded(grad_norms, jnp.maximum)
        if t < ITERS:
            active = mask[t : t + 1, cols(x)].astype(F32)
            pruned.append(1.0 - active)
            moved = current[...] + step_sizes * gradient
            moved_norms = column_norms(moved)
            cutoff = step_sizes * penalty
            factor = jnp.maximum(moved_norms - cutoff, 0.0) / jnp.maximum(moved_norms, cutoff)
            updated = (active * factor) * moved
            flipped = updated.T
            half[t + 1, x] = flipped.astype(BF16)
            own_half = half.at[t + 1, x]
            h1 = halved(own_half, own_half, {"x": xf}, quarter)
            h2 = send(own_half, own_half, {"x": xb})
            current[...] = updated
            bn.append(column_norms(updated))
            if t == ITERS - 1:
                coef_parts[x] = flipped
            h3 = []
            for h in range(2):
                h1[h].wait_recv()
                through = half.at[t + 1, xb, pl.ds(h * quarter // 2, quarter // 2)]
                h3.append(send(through, through, {"x": xf}))
            h2.wait_recv()
            waited(h3)
            if t == ITERS - 1:
                own_coef = coef_parts.at[x]
                coef_copies = [send(own_coef, own_coef, {"x": xq}) for xq in (xf, xb, x2)]

    for i, value in enumerate(rr + ry):
        stats[i : i + 1, :] = value
    for i, value in enumerate(bn + pruned):
        stats[6 + i : 7 + i, :] = lanes_folded(value, jnp.add)
    stats[11:16, :] = jnp.zeros((5, 128), F32)
    stats[19:24, :] = jnp.zeros((5, 128), F32)
    norms[x, 3:8, :] = jnp.zeros((5, quarter), F32)
    own_norms = norms.at[x]
    norm_copies = [send(own_norms, own_norms, {"x": xq}) for xq in (xf, xb, x2)]
    lane = lax.broadcasted_iota(jnp.int32, (24, 128), 1)
    row = lax.broadcasted_iota(jnp.int32, (24, 128), 0)
    sums = jnp.sum(stats[...], axis=1, keepdims=True)
    tops = jnp.max(stats[...], axis=1, keepdims=True)
    fin_src[0] = jnp.zeros((8, 128), F32)
    fin_src[1] = jnp.zeros((8, 128), F32)
    fin_src[0, 0:1, :] = jnp.sum(jnp.where((lane == row) & (row < 16), sums, 0.0), axis=0, keepdims=True)
    fin_src[0, 1:2, :] = jnp.sum(jnp.where(lane == row - 16, tops, 0.0), axis=0, keepdims=True)
    for k, (arrived, group) in enumerate(((fin_plane, plane), (fin_column, column))):
        copies = [send(fin_src.at[k], arrived.at[i], peer) for i, peer in enumerate(group)]
        if k == 0:
            waited(coef_copies)
            for q in range(NX):
                coef[q * quarter : (q + 1) * quarter, :] = coef_parts[q]
        waited(copies)
        sums, tops = fin_src[k, 0:1, :], fin_src[k, 1:2, :]
        for d in range(len(group)):
            sums = sums + arrived[d, 0:1, :]
            tops = jnp.maximum(tops, arrived[d, 1:2, :])
        if k == 0:
            fin_src[1, 0:1, :] = sums
            fin_src[1, 1:2, :] = tops
    waited(norm_copies)
    for t in range(ITERS + 1):
        scale = jnp.maximum(penalty, tops[:, t : t + 1])
        for q in range(NX):
            corr[t : t + 1, q * quarter : (q + 1) * quarter] = norms[q, t : t + 1, :] / scale
        rr_sum, ry_sum, bn_sum = (sums[:, i : i + 1] for i in (t, 3 + t, 6 + t))
        primal = 0.5 * rr_sum + penalty * bn_sum
        ratio = penalty / scale
        dual = ratio * ry_sum - 0.5 * ratio * ratio * rr_sum
        gaps[t] = jnp.sum((primal - dual) / (primal + 1.0))
    for t in range(ITERS):
        counts[t] = jnp.sum(sums[:, 9 + t : 10 + t])
    drain()
    assert used[0] == send_sem.shape[0], used[0]


def hand_over(coef_in, corr_in, gaps_in, counts_in, coef, corr, gaps, counts):
    coef[...] = coef_in[...]
    corr[...] = corr_in[...]
    for t in range(ITERS + 1):
        gaps[t] = gaps_in[t]
    for t in range(ITERS):
        counts[t] = counts_in[t]


def local(design, targets, warm_start, active_mask, penalty_index):
    samples, features = design.shape
    tasks = targets.shape[1]
    block = samples // (2 * NY)
    sub = block // NZ
    quarter = features // NX
    steps = ITERS + 1
    vmem, smem, hbm = pltpu.VMEM, pltpu.SMEM, pl.ANY
    target_blocks = targets.reshape(2 * NY * NZ, sub, tasks)
    scratch = [
        vmem((samples, features), BF16),
        vmem((samples, tasks), BF16),
        vmem((sub, tasks), BF16),
        vmem((steps, NX, quarter, tasks), BF16),
        vmem((4, block, tasks), F32),
        vmem((steps, 4, block, tasks), F32),
        tuple(vmem((3, block, tasks), v) for v in Y_TYPES),
        tuple(vmem((3, block, tasks), v) for v in Y_TYPES),
        vmem((2, block, tasks), F32),
        vmem((NZ, sub, tasks), F32),
        tuple(vmem((NZ, sub, tasks), v) for v in Z_TYPES),
        tuple(vmem((NZ - 1, sub, tasks), v) for v in Z_TYPES),
        vmem((steps, 2, NY, NZ, sub, tasks), BF16),
        vmem((tasks, features), F32),
        tuple(vmem((3, tasks, quarter), v) for v in X_TYPES),
        tuple(vmem((3, tasks, quarter), v) for v in X_TYPES),
        vmem((tasks, quarter), F32),
        vmem((NX, quarter, tasks), F32),
        vmem((NX, 8, quarter), F32),
        vmem((NX - 1, 8, quarter), F32),
        vmem((4, 8, 128), F32),
        vmem((NZ - 1, 8, 128), F32),
        vmem((NY - 1, 8, 128), F32),
        vmem((1, 8, 128), F32),
        vmem((NX - 1, 8, 128), F32),
        vmem((NX, 8, quarter), F32),
        vmem((2, 8, 128), F32),
        vmem((NX * NY - 1, 8, 128), F32),
        vmem((2 * NZ - 1, 8, 128), F32),
        vmem((24, 128), F32),
        pltpu.SemaphoreType.DMA((10,)),
        pltpu.SemaphoreType.DMA((257,)),
        pltpu.SemaphoreType.DMA((257,)),
    ]
    out_shape = (
        jax.ShapeDtypeStruct((features, tasks), F32),
        jax.ShapeDtypeStruct((steps, features), F32),
        jax.ShapeDtypeStruct((steps,), F32),
        jax.ShapeDtypeStruct((ITERS,), F32),
    )
    results = tuple(pl.BlockSpec(memory_space=m) for m in (vmem, vmem, smem, smem))
    found = pl.pallas_call(
        kernel,
        out_shape=out_shape,
        in_specs=[pl.BlockSpec(memory_space=m) for m in (hbm, hbm, hbm, vmem, vmem, smem)],
        out_specs=results,
        scratch_shapes=scratch,
        compiler_params=pltpu.CompilerParams(
            collective_id=0, has_side_effects=True, vmem_limit_bytes=56 * 1024 * 1024
        ),
        name="lasso_steps",
    )(design, targets, target_blocks, warm_start, active_mask, penalty_index)
    return pl.pallas_call(
        hand_over, out_shape=out_shape, in_specs=list(results), out_specs=results, name="hand_over"
    )(*found)


def solution(mesh):
    torus = Mesh(mesh.devices.reshape(NY, NZ, 2, NX), ("y", "z", "c", "x"))
    feat = ("y", "z", "c")
    in_specs = (P("x", feat), P("x", None), P(feat, None), P(None, feat), P())
    out_specs = (P(feat, None), P(None, feat), P(), P())
    return jax.shard_map(local, mesh=torus, in_specs=in_specs, out_specs=out_specs, check_vma=False)
```

```python
import jax
import jax.numpy as jnp
from jax import lax
from jax.experimental import pallas as pl
from jax.experimental.pallas import tpu as pltpu
from jax.sharding import Mesh
from jax.sharding import PartitionSpec as P

ITERS = 2
NY, NZ, NX = 4, 8, 4
MESH = pl.DeviceIdType.MESH
PIECES = 4
FAR_FIRST = (4, 3, 5, 2, 6, 1, 7)
F32 = jnp.float32
BF16 = jnp.bfloat16
Y_TYPES = (BF16, F32, BF16)
Z_TYPES = (BF16, F32, BF16)
X_TYPES = (F32, F32, BF16, BF16)


def lanes_folded(row, op):
    return op(row[:, :128], row[:, 128:])


def column_norms(matrix):
    return jnp.sqrt(jnp.sum(matrix * matrix, axis=0, keepdims=True))


def kernel(
    design, targets, target_blocks, warm, mask, penalty_index,
    coef, corr, gaps, counts,
    D, T, own_targets, half, cs, cr, ys, yr, keep, zt, zs, zr, R, G, gs, gr,
    current, coef_parts, cqs, cqr, pen_src, pen_z, pen_y, pen_c, pen_x,
    norms, fin_src, fin_plane, fin_column, stats, load_sem, send_sem, recv_sem,
):
    y, z, c, x = (lax.axis_index(a) for a in ("y", "z", "c", "x"))
    oc = 1 - c
    step = 1 - 2 * c
    yf, yb, y2 = lax.rem(y + step + NY, NY), lax.rem(y - step + NY, NY), lax.rem(y + 2, NY)
    xf, xb, x2 = lax.rem(x + step + NX, NX), lax.rem(x - step + NX, NX), lax.rem(x + 2, NX)
    block = D.shape[0] // (2 * NY)
    quarter = D.shape[1] // NX
    sub = block // NZ
    task_count = warm.shape[1]

    def rows(cc, yy):
        return pl.ds(pl.multiple_of((cc * NY + yy) * block, block), block)

    def cols(xx):
        return pl.ds(pl.multiple_of(xx * quarter, quarter), quarter)

    used = [0]
    pending = []

    def send(src, dst, device):
        i = used[0]
        used[0] += 1
        copy = pltpu.make_async_remote_copy(
            src_ref=src, dst_ref=dst, send_sem=send_sem.at[i], recv_sem=recv_sem.at[i],
            device_id=device, device_id_type=MESH,
        )
        copy.start()
        pending.append(copy)
        return copy

    def drain():
        for copy in pending:
            copy.wait_send()
        pending.clear()

    def to_all(src, dst, axis, me, n):
        return [
            send(src, dst.at[d - 1], {axis: lax.rem(me + d, n)}) for d in range(1, n)
        ]

    def waited(copies):
        for copy in copies:
            copy.wait_recv()

    others, mine = (y2, yf, yb, y), (y2, yb, yf, y)
    steps = (("o", 0), ("o", 1), ("m", 0), ("o", 2), ("m", 1), ("o", 3), ("m", 2), ("m", 3))
    loads = {}
    for i, (kind, j) in enumerate(steps):
        cc, yy = (oc, others[j]) if kind == "o" else (c, mine[j])
        load = pltpu.make_async_copy(design.at[rows(cc, yy), :], D.at[rows(cc, yy), :], load_sem.at[i])
        load.start()
        loads[kind, j] = load
    own_load = pltpu.make_async_copy(
        target_blocks.at[(c * NY + y) * NZ + z], own_targets, load_sem.at[8]
    )
    own_load.start()
    target_load = pltpu.make_async_copy(targets, T, load_sem.at[9])
    target_load.start()

    barrier = pltpu.get_barrier_semaphore()
    peers = (
        [{"c": oc}]
        + [{"y": lax.rem(y + d, NY)} for d in range(1, NY)]
        + [{"z": lax.rem(z + d, NZ)} for d in range(1, NZ)]
        + [{"x": lax.rem(x + d, NX)} for d in range(1, NX)]
    )
    plane = [
        {"x": lax.rem(x + d, NX), "y": lax.rem(y + e, NY)}
        for d in range(NX) for e in range(NY) if d or e
    ]
    column = [
        {"z": lax.rem(z + d, NZ), "c": lax.rem(c + e, 2)} for d in range(NZ) for e in range(2) if d or e
    ]
    peers += [
        {"x": lax.rem(x + d, NX), "y": lax.rem(y + e, NY)} for d in range(1, NX) for e in range(1, NY)
    ]
    peers += [{"z": lax.rem(z + d, NZ), "c": oc} for d in range(1, NZ)]
    for peer in peers:
        pl.semaphore_signal(barrier, inc=1, device_id=peer, device_id_type=MESH)

    half[0] = warm[...].astype(BF16).reshape(half.shape[1:])
    current[...] = warm[cols(x), :].T
    bn = [column_norms(current[...])]

    def grad_block(R_t, cc, yy, first):
        part = R_t[cc, yy].astype(F32).reshape(block, task_count).astype(BF16)
        product = lax.dot_general(
            part, D[rows(cc, yy), :], (((0,), (0,)), ((), ())), preferred_element_type=F32
        )
        if first:
            G[...] = product
        else:
            G[...] += product

    task_parts = [pl.ds(h * task_count // PIECES, task_count // PIECES) for h in range(PIECES)]

    def ring_start(k):
        gs[k][0] = G[:, cols(x2)].astype(X_TYPES[k])
        a = [send(gs[k].at[0, p], gr[k].at[0, p], {"x": xf}) for p in task_parts]
        gs[k][1] = G[:, cols(xb)].astype(X_TYPES[k])
        b = send(gs[k].at[1], gr[k].at[1], {"x": xb})
        return a, b

    def ring_middle(k, a):
        last = []
        for copy, p in zip(a, task_parts):
            copy.wait_recv()
            gs[k][2, p, :] = (G[p, cols(xf)] + gr[k][0, p, :].astype(F32)).astype(X_TYPES[k])
            last.append(send(gs[k].at[2, p], gr[k].at[2, p], {"x": xf}))
        return last

    def ring_end(k, b, last):
        b.wait_recv()
        waited(last)
        return G[:, cols(x)] + gr[k][1].astype(F32) + gr[k][2].astype(F32)

    def maximum_of(src, arrived):
        value = src
        for d in range(arrived.shape[0]):
            value = jnp.maximum(value, arrived[d])
        return value

    penalty = step_sizes = None
    coef_copies = []
    rr, ry, pruned = [], [], []
    for t in range(ITERS + 1):
        weights = half[t].reshape(D.shape[1], task_count).astype(F32).T.astype(BF16)

        def product(cc, yy):
            turned = lax.dot_general(
                weights, D[rows(cc, yy), :], (((1,), (1,)), ((), ())), preferred_element_type=F32
            )
            return turned.T

        core_copies = []

        def in_pieces(src, dst, device, length):
            parts = [pl.ds(h * length // PIECES, length // PIECES) for h in range(PIECES)]
            return [send(src.at[p], dst.at[p], device) for p in parts]

        def other(j):
            if t == 0:
                loads["o", j].wait()
            cs[j] = product(oc, others[j])
            if t == 0 and j == 0:
                pl.semaphore_wait(barrier, len(peers))
            core_copies.append(send(cs.at[j], cr.at[t, j], {"c": oc}))

        def summed(j):
            if t == 0:
                loads["m", j].wait()
            own = product(c, mine[j])
            core_copies[j].wait_recv()
            return own + cr[t, j]

        other(0)
        other(1)
        ys[t][0] = summed(0).astype(Y_TYPES[t])
        ya = in_pieces(ys[t].at[0], yr[t].at[0], {"y": yf}, block)
        other(2)
        ys[t][1] = summed(1).astype(Y_TYPES[t])
        yb_copy = send(ys[t].at[1], yr[t].at[1], {"y": yb})
        other(3)
        keep[0] = summed(2)
        keep[1] = summed(3)
        if t == 0:
            target_load.wait()
            for b in range(2 * NY):
                part = T[b * block : (b + 1) * block, :]
                corr_product = lax.dot_general(
                    part, D[b * block : (b + 1) * block, :], (((0,), (0,)), ((), ())),
                    preferred_element_type=F32,
                )
                if b == 0:
                    G[...] = corr_product
                else:
                    G[...] += corr_product
            ca, cb = ring_start(ITERS + 1)
        yc = []
        for h in range(PIECES):
            ya[h].wait_recv()
            p = pl.ds(h * block // PIECES, block // PIECES)
            ys[t][2, p, :] = (keep[0, p, :] + yr[t][0, p, :].astype(F32)).astype(Y_TYPES[t])
            yc.append(send(ys[t].at[2, p], yr[t].at[2, p], {"y": yf}))
        if t == 0:
            def square_step(i, total):
                v = D[pl.ds(pl.multiple_of(i * 64, 64), 64), :].astype(F32)
                return total + jnp.sum((v * v).reshape(8, 8, v.shape[1]), axis=0)

            squares = lax.fori_loop(
                0, D.shape[0] // 64, square_step, jnp.zeros((8, D.shape[1]), F32)
            )
            squares = jnp.sum(squares, axis=0, keepdims=True)
            for q in range(NX):
                cqs[q] = jnp.broadcast_to(squares[:, q * quarter : (q + 1) * quarter], (8, quarter))
            square_copies = [
                send(cqs.at[lax.rem(x + d, NX)], cqr.at[d - 1], {"x": lax.rem(x + d, NX)})
                for d in range(1, NX)
            ]
            cc_copy = ring_middle(ITERS + 1, ca)
        yb_copy.wait_recv()
        waited(yc)
        total = (keep[1] + yr[t][1].astype(F32) + yr[t][2].astype(F32)).reshape(NZ, sub, task_count)
        zt[...] = total
        zs[t][...] = total.astype(Z_TYPES[t])
        z_copies = []
        for d in FAR_FIRST:
            zz = lax.rem(z + d, NZ)
            z_copies.append(send(zs[t].at[zz], zr[t].at[d - 1], {"z": zz}))
        if t == 0:
            corr_y = ring_end(ITERS + 1, cb, cc_copy)
            top = lanes_folded(column_norms(corr_y), jnp.maximum)
            pen_src[0] = jnp.broadcast_to(top, (8, 128))
            pen_copies = to_all(pen_src.at[0], pen_z, "z", z, NZ)
            own_load.wait()
        waited(z_copies)
        fitted = zt[z]
        for d in range(NZ - 1):
            fitted = fitted + zr[t][d].astype(F32)
        target_float = own_targets[...].astype(F32)
        residual = (target_float - fitted).astype(BF16)
        R[t, c, y, z] = residual
        own_rows = R.at[t, c, y, z]
        r_copies = [send(own_rows, own_rows, {"z": lax.rem(z + d, NZ)}) for d in FAR_FIRST]
        resid_float = residual.astype(F32)
        rr.append(jnp.sum(resid_float * resid_float, axis=0, keepdims=True))
        ry.append(jnp.sum(resid_float * target_float, axis=0, keepdims=True))
        near_first = (0, *reversed(FAR_FIRST))
        g1, g2 = [], []
        for d in near_first:
            if d:
                r_copies[FAR_FIRST.index(d)].wait_recv()
            through = R.at[t, c, y, lax.rem(z - d + NZ, NZ)]
            g1.append(send(through, through, {"y": yf}))
            g2.append(send(through, through, {"y": yb}))

        def block_to(yy, device):
            return send(R.at[t, c, yy], R.at[t, c, yy], device)

        R_t = R.at[t]
        q0 = block_to(y, {"c": oc})
        if t == 0:
            waited(pen_copies)
            pen_src[1] = maximum_of(pen_src[0], pen_z)
            pen_copies = to_all(pen_src.at[1], pen_y, "y", y, NY)
        grad_block(R_t, c, y, True)
        q0.wait_recv()
        grad_block(R_t, oc, y, False)
        g3 = []
        for d, copy in zip(near_first, g1):
            copy.wait_recv()
            through = R.at[t, c, yb, lax.rem(z - d + NZ, NZ)]
            g3.append(send(through, through, {"y": yf}))
        q1 = block_to(yb, {"c": oc})
        waited(g2)
        q2 = block_to(yf, {"c": oc})
        if t == 0:
            waited(pen_copies)
            pen_src[2] = maximum_of(pen_src[1], pen_y)
            pen_copies = to_all(pen_src.at[2], pen_c, "c", c, 2)
        grad_block(R_t, c, yb, False)
        grad_block(R_t, c, yf, False)
        q1.wait_recv()
        grad_block(R_t, oc, yf, False)
        q3 = []
        for d, copy in zip(near_first, g3):
            copy.wait_recv()
            through = R.at[t, c, y2, lax.rem(z - d + NZ, NZ)]
            q3.append(send(through, through, {"c": oc}))
        q2.wait_recv()
        grad_block(R_t, oc, yb, False)
        grad_block(R_t, c, y2, False)
        waited(q3)
        grad_block(R_t, oc, y2, False)
        ga, gb = ring_start(t)
        if t == 0:
            waited(pen_copies)
            pen_src[3] = maximum_of(pen_src[2], pen_c)
            pen_copies = to_all(pen_src.at[3], pen_x, "x", x, NX)
        gc = ring_middle(t, ga)
        if t == 0:
            waited(pen_copies)
            pen_max = jnp.max(maximum_of(pen_src[3], pen_x), axis=(0, 1), keepdims=True)
            penalty = pen_max / (8.0 + 4.0 * penalty_index[0].astype(F32))
            waited(square_copies)
            total_squares = (cqs[x] + cqr[0] + cqr[1] + cqr[2])[0:1, :]
            step_sizes = 0.5 / (1.0 + total_squares)
        gradient = ring_end(t, gb, gc)
        drain()
        grad_norms = column_norms(gradient)
        norms[x, t : t + 1, :] = grad_norms
        stats[16 + t : 17 + t, :] = lanes_folded(grad_norms, jnp.maximum)
        if t < ITERS:
            active = mask[t : t + 1, cols(x)].astype(F32)
            pruned.append(1.0 - active)
            moved = current[...] + step_sizes * gradient
            moved_norms = column_norms(moved)
            cutoff = step_sizes * penalty
            factor = jnp.maximum(moved_norms - cutoff, 0.0) / jnp.maximum(moved_norms, cutoff)
            updated = (active * factor) * moved
            flipped = updated.T
            half[t + 1, x] = flipped.astype(BF16)
            own_half = half.at[t + 1, x]
            h1 = in_pieces(own_half, own_half, {"x": xf}, quarter)
            h2 = send(own_half, own_half, {"x": xb})
            current[...] = updated
            bn.append(column_norms(updated))
            if t == ITERS - 1:
                coef_parts[x] = flipped
            h3 = []
            for h in range(PIECES):
                h1[h].wait_recv()
                through = half.at[t + 1, xb, pl.ds(h * quarter // PIECES, quarter // PIECES)]
                h3.append(send(through, through, {"x": xf}))
            h2.wait_recv()
            waited(h3)
            if t == ITERS - 1:
                own_coef = coef_parts.at[x]
                coef_copies = [send(own_coef, own_coef, {"x": xq}) for xq in (xf, xb, x2)]

    for i, value in enumerate(rr + ry):
        stats[i : i + 1, :] = value
    for i, value in enumerate(bn + pruned):
        stats[6 + i : 7 + i, :] = lanes_folded(value, jnp.add)
    stats[11:16, :] = jnp.zeros((5, 128), F32)
    stats[19:24, :] = jnp.zeros((5, 128), F32)
    norms[x, 3:8, :] = jnp.zeros((5, quarter), F32)
    own_norms = norms.at[x]
    norm_copies = [send(own_norms, own_norms, {"x": xq}) for xq in (xf, xb, x2)]
    lane = lax.broadcasted_iota(jnp.int32, (24, 128), 1)
    row = lax.broadcasted_iota(jnp.int32, (24, 128), 0)
    sums = jnp.sum(stats[...], axis=1, keepdims=True)
    tops = jnp.max(stats[...], axis=1, keepdims=True)
    fin_src[0] = jnp.zeros((8, 128), F32)
    fin_src[1] = jnp.zeros((8, 128), F32)
    fin_src[0, 0:1, :] = jnp.sum(jnp.where((lane == row) & (row < 16), sums, 0.0), axis=0, keepdims=True)
    fin_src[0, 1:2, :] = jnp.sum(jnp.where(lane == row - 16, tops, 0.0), axis=0, keepdims=True)
    for k, (arrived, group) in enumerate(((fin_plane, plane), (fin_column, column))):
        copies = [send(fin_src.at[k], arrived.at[i], peer) for i, peer in enumerate(group)]
        if k == 0:
            waited(coef_copies)
            for q in range(NX):
                coef[q * quarter : (q + 1) * quarter, :] = coef_parts[q]
        waited(copies)
        sums, tops = fin_src[k, 0:1, :], fin_src[k, 1:2, :]
        for d in range(len(group)):
            sums = sums + arrived[d, 0:1, :]
            tops = jnp.maximum(tops, arrived[d, 1:2, :])
        if k == 0:
            fin_src[1, 0:1, :] = sums
            fin_src[1, 1:2, :] = tops
    waited(norm_copies)
    for t in range(ITERS + 1):
        scale = jnp.maximum(penalty, tops[:, t : t + 1])
        for q in range(NX):
            corr[t : t + 1, q * quarter : (q + 1) * quarter] = norms[q, t : t + 1, :] / scale
        rr_sum, ry_sum, bn_sum = (sums[:, i : i + 1] for i in (t, 3 + t, 6 + t))
        primal = 0.5 * rr_sum + penalty * bn_sum
        ratio = penalty / scale
        dual = ratio * ry_sum - 0.5 * ratio * ratio * rr_sum
        gaps[t] = jnp.sum((primal - dual) / (primal + 1.0))
    for t in range(ITERS):
        counts[t] = jnp.sum(sums[:, 9 + t : 10 + t])
    drain()
    assert used[0] == send_sem.shape[0], used[0]


def hand_over(coef_in, corr_in, gaps_in, counts_in, coef, corr, gaps, counts):
    coef[...] = coef_in[...]
    corr[...] = corr_in[...]
    for t in range(ITERS + 1):
        gaps[t] = gaps_in[t]
    for t in range(ITERS):
        counts[t] = counts_in[t]


def local(design, targets, warm_start, active_mask, penalty_index):
    samples, features = design.shape
    tasks = targets.shape[1]
    block = samples // (2 * NY)
    sub = block // NZ
    quarter = features // NX
    steps = ITERS + 1
    vmem, smem, hbm = pltpu.VMEM, pltpu.SMEM, pl.ANY
    target_blocks = targets.reshape(2 * NY * NZ, sub, tasks)
    scratch = [
        vmem((samples, features), BF16),
        vmem((samples, tasks), BF16),
        vmem((sub, tasks), BF16),
        vmem((steps, NX, quarter, tasks), BF16),
        vmem((4, block, tasks), F32),
        vmem((steps, 4, block, tasks), F32),
        tuple(vmem((3, block, tasks), v) for v in Y_TYPES),
        tuple(vmem((3, block, tasks), v) for v in Y_TYPES),
        vmem((2, block, tasks), F32),
        vmem((NZ, sub, tasks), F32),
        tuple(vmem((NZ, sub, tasks), v) for v in Z_TYPES),
        tuple(vmem((NZ - 1, sub, tasks), v) for v in Z_TYPES),
        vmem((steps, 2, NY, NZ, sub, tasks), BF16),
        vmem((tasks, features), F32),
        tuple(vmem((3, tasks, quarter), v) for v in X_TYPES),
        tuple(vmem((3, tasks, quarter), v) for v in X_TYPES),
        vmem((tasks, quarter), F32),
        vmem((NX, quarter, tasks), F32),
        vmem((NX, 8, quarter), F32),
        vmem((NX - 1, 8, quarter), F32),
        vmem((4, 8, 128), F32),
        vmem((NZ - 1, 8, 128), F32),
        vmem((NY - 1, 8, 128), F32),
        vmem((1, 8, 128), F32),
        vmem((NX - 1, 8, 128), F32),
        vmem((NX, 8, quarter), F32),
        vmem((2, 8, 128), F32),
        vmem((NX * NY - 1, 8, 128), F32),
        vmem((2 * NZ - 1, 8, 128), F32),
        vmem((24, 128), F32),
        pltpu.SemaphoreType.DMA((10,)),
        pltpu.SemaphoreType.DMA((293,)),
        pltpu.SemaphoreType.DMA((293,)),
    ]
    out_shape = (
        jax.ShapeDtypeStruct((features, tasks), F32),
        jax.ShapeDtypeStruct((steps, features), F32),
        jax.ShapeDtypeStruct((steps,), F32),
        jax.ShapeDtypeStruct((ITERS,), F32),
    )
    results = tuple(pl.BlockSpec(memory_space=m) for m in (vmem, vmem, smem, smem))
    found = pl.pallas_call(
        kernel,
        out_shape=out_shape,
        in_specs=[pl.BlockSpec(memory_space=m) for m in (hbm, hbm, hbm, vmem, vmem, smem)],
        out_specs=results,
        scratch_shapes=scratch,
        compiler_params=pltpu.CompilerParams(
            collective_id=0, has_side_effects=True, vmem_limit_bytes=56 * 1024 * 1024
        ),
        name="lasso_steps",
    )(design, targets, target_blocks, warm_start, active_mask, penalty_index)
    return pl.pallas_call(
        hand_over, out_shape=out_shape, in_specs=list(results), out_specs=results, name="hand_over"
    )(*found)


def solution(mesh):
    torus = Mesh(mesh.devices.reshape(NY, NZ, 2, NX), ("y", "z", "c", "x"))
    feat = ("y", "z", "c")
    in_specs = (P("x", feat), P("x", None), P(feat, None), P(None, feat), P())
    out_specs = (P(feat, None), P(None, feat), P(), P())
    return jax.shard_map(local, mesh=torus, in_specs=in_specs, out_specs=out_specs, check_vma=False)
```
